128 devices in a mesh: row: 8 (over z, x_lo), col: 16 (over y, x_hi, core).
Axes of the slice: x: 4 (x_hi: 2, x_lo: 2; x = x_hi * 2 + x_lo), y: 4, z: 4, core: 2. Of those that a mesh axis runs over, the one named last changes fastest.
Arguments:
- tokens: bfloat16 [256, 16384], P('row', 'col'), may hold values from -6 to 6
- probe_words: int32 [256, 512], P(None, 'col'), may hold values from -2147483648 to 2147483646, as said below
- token_ids: int32 [256], replicated, may hold values from 0 to 128255
- loss_weight: float32 [128256], replicated, may hold values from 0.5 to 2
- gate_weight: bfloat16 [16384, 26624], P('col', 'row'), may hold values from -0.046875 to 0.046875
- up_weight: bfloat16 [16384, 26624], P('col', 'row'), may hold values from -0.046875 to 0.046875
- down_weight: bfloat16 [26624, 16384], P('row', 'col'), may hold values from -0.0390625 to 0.0390625
Outputs:
- hvp: float32 [256, 16384], P('row', 'col')
The draws below stay inside these ranges and needn't reach their ends.
Inputs may be any that keep to these rules, and one draw needn't show every extreme that they name: `probe_words`: every bit of every word is an independent fair sign bit; bit k of word j of token t is the probe sign of feature 32 j + k of that token (set: +1, clear: -1).
All inputs are finite; a program needn't handle non-finite values.
Results may differ from the reference program's by a relative error of at most 0.0036.
Values may be sent and summed in bfloat16 or wider, within the bound.
No kernel may reach another device: no remote copies, remote signals or barrier semaphores. Data moves between devices by JAX's collectives and lax.ppermute only.
A program may use at most 128 MiB of HBM per device.

```python
import math
import jax
import jax.numpy as jnp
import numpy as np
from jax import lax

D = 16384
FF = 26624
VOCAB = 128256
TOKENS = 256


def draw_probe_words(key, part):
    return jax.random.randint(key, (TOKENS, D // 32), -2147483648, 2147483647, dtype=jnp.int32)


def touch_ends(values, stream_key, smallest, top_value):
    place = [jax.random.randint(jax.random.fold_in(stream_key, axis), (), 0, length) for axis, length in enumerate(values.shape)]
    widest = values.shape.index(max(values.shape))
    neighbour = place[:widest] + [(place[widest] + 1) % values.shape[widest]] + place[widest + 1:]
    return values.at[tuple(place)].set(smallest).at[tuple(neighbour)].set(top_value)


def level_of(stream_key, extent, split, least, high):
    factor_of, own = 1.0, jax.random.fold_in(stream_key, 6)
    for position, parts in split:
        draws = jnp.exp(jax.random.uniform(jax.random.fold_in(own, position), (parts,), jnp.float32, least / len(split), high / len(split)))
        factor_of = factor_of * jnp.repeat(draws, extent[position] // parts).reshape([-1 if axis == position else 1 for axis in range(len(extent))])
    return factor_of


def ranked_wide(key, extent, count, lean):
    weights = [min(1 << octave, count + 1 - (1 << octave)) * (1 << 20) // math.isqrt((1 << octave) ** lean) + 1 for octave in range((count + 1).bit_length()) if 1 << octave <= count]
    scale = 1 + sum(weights) // (1 << 30)
    table = np.cumsum(np.array([max(1, weight // scale) for weight in weights]))
    pick = jax.random.randint(jax.random.fold_in(key, 1), extent, 0, int(table[len(weights) - 1]))
    start = jnp.left_shift(1, jnp.searchsorted(jnp.asarray(table, jnp.int32), pick, side="right").astype(jnp.int32))
    rank = start - 1 + jax.random.randint(jax.random.fold_in(key, 4), extent, 0, 1 << 30) % jnp.minimum(start, count + 1 - start)
    return jax.random.permutation(jax.random.fold_in(key, 2), count)[rank].astype(jnp.int32)


def gaussian(stream_key, shape, width, limit, cuts=(), kind=jnp.bfloat16):
    result = jax.random.normal(stream_key, shape, jnp.float32) * width
    if len(cuts) > 0:
        result = level_of(stream_key, shape, cuts, -0.22, 0.18) * result
    return jnp.clip(result, min=-limit, max=limit).astype(kind)


def setup_inputs(seed: int = 0) -> dict:
    key_of = jax.random.split(jax.random.key(seed), 8)
    tokens = gaussian(key_of[0], (TOKENS, D), 1.0, 6.0, ((0, 8), (1, 16)))
    probe_words = draw_probe_words(jax.random.fold_in(key_of[7], 71), 0)
    token_ids = touch_ends(ranked_wide(key_of[2], (TOKENS,), VOCAB, 2), jax.random.fold_in(key_of[2], 3), 0, VOCAB - 1).astype(jnp.int32)
    loss_weight = jnp.clip(jnp.exp(jax.random.uniform(key_of[3], (VOCAB,), jnp.float32, math.log(0.5), math.log(2.0))), 0.5, 2.0)
    gate_weight = gaussian(key_of[4], (D, FF), D ** -0.5, 0.046875, ((0, 16), (1, 8)))
    up_weight = gaussian(key_of[5], (D, FF), D ** -0.5, 0.046875, ((0, 16), (1, 8)))
    down_weight = gaussian(key_of[6], (FF, D), FF ** -0.5, 0.0390625, ((0, 8), (1, 16)))
    return dict(tokens=tokens, probe_words=probe_words, token_ids=token_ids, loss_weight=loss_weight, gate_weight=gate_weight, up_weight=up_weight, down_weight=down_weight)


def unpack_signs(packed):
    shifts = jnp.arange(32, dtype=jnp.int32)
    bit_vals = jnp.bitwise_and(jnp.right_shift(packed[:, :, None], shifts), 1)
    return (2 * bit_vals - 1).reshape(packed.shape[0], -1).astype(jnp.bfloat16)


def silu_parts(pre_act):
    sigmoid_pre = jax.nn.sigmoid(pre_act)
    active = pre_act * sigmoid_pre
    slopes = sigmoid_pre * (1.0 + pre_act * (1.0 - sigmoid_pre))
    curves = sigmoid_pre * (1.0 - sigmoid_pre) * (2.0 + pre_act * (1.0 - 2.0 * sigmoid_pre))
    return active, slopes, curves


def matmul(left_rows, weight):
    return jnp.dot(left_rows, weight, preferred_element_type=jnp.float32)


def matmul_trans(left_rows, weight):
    return lax.dot_general(left_rows, weight, (((1,), (1,)), ((), ())), preferred_element_type=jnp.float32)


def reference(tokens, probe_words, token_ids, loss_weight, gate_weight, up_weight, down_weight):
    probe = unpack_signs(probe_words)
    gate_pre = matmul(tokens, gate_weight)
    up_pre = matmul(tokens, up_weight)
    gate_tan = matmul(probe, gate_weight)
    up_tan = matmul(probe, up_weight)
    active, slopes, curves = silu_parts(gate_pre)
    hidden = (active * up_pre).astype(jnp.bfloat16)
    hidden_tan = (slopes * gate_tan * up_pre + active * up_tan).astype(jnp.bfloat16)
    output = matmul(hidden, down_weight)
    out_tan = matmul(hidden_tan, down_weight)
    weight_tok = jnp.take(loss_weight, token_ids)[:, None]
    cotangent = (weight_tok * (tokens.astype(jnp.float32) + output)).astype(jnp.bfloat16)
    cot_tan = weight_tok * (probe.astype(jnp.float32) + out_tan)
    cot_half = cot_tan.astype(jnp.bfloat16)
    backward = matmul_trans(cotangent, down_weight)
    back_tan = matmul_trans(cot_half, down_weight)
    gate_back = (back_tan * up_pre * slopes + backward * up_tan * slopes + backward * up_pre * curves * gate_tan).astype(jnp.bfloat16)
    up_back = (back_tan * active + backward * slopes * gate_tan).astype(jnp.bfloat16)
    return cot_tan + matmul_trans(gate_back, gate_weight) + matmul_trans(up_back, up_weight)
```

```python
import jax
import jax.numpy as jnp
from jax import lax
from jax.sharding import PartitionSpec as P

BF16 = jnp.bfloat16
F16 = jnp.float16
F32 = jnp.float32

SWAP_CORE = [(c, c ^ 1) for c in range(16)]
SWAP_HI = [(c, c ^ 2) for c in range(16)]
SWAP_LO = [(r, r ^ 1) for r in range(8)]


def shift_y(x, d):
    return lax.ppermute(x, "col", [(c, (c + 4 * d) % 16) for c in range(16)])


def shift_z(x, d):
    return lax.ppermute(x, "row", [(r, (r + 2 * d) % 8) for r in range(8)])


def swap_core(x):
    return lax.ppermute(x, "col", SWAP_CORE)


def swap_hi(x):
    return lax.ppermute(x, "col", SWAP_HI)


def swap_lo(x):
    return lax.ppermute(x, "row", SWAP_LO)


def pick(x, i, axis=0):
    return lax.dynamic_index_in_dim(x, i, axis, keepdims=False)


def scatter_sum(x, shift, place, narrow):
    total = pick(x, place(0)).astype(F32)
    arrived = [shift(pick(x, place(d)).astype(narrow), d) for d in (1, 3, 2)]
    for a in arrived:
        total = total + a.astype(F32)
    return total


def gather_ring(x, shift):
    got = {d: shift(x, d) for d in (1, 3, 2)}
    return jnp.stack([x, got[3], got[2], got[1]])


def unpack_signs(packed):
    shifts = jnp.arange(32, dtype=jnp.int32)
    bit_vals = jnp.bitwise_and(jnp.right_shift(packed[:, :, None], shifts), 1)
    return (2 * bit_vals - 1).reshape(packed.shape[0], -1).astype(BF16)


def silu_parts(pre_act):
    sigmoid_pre = jax.nn.sigmoid(pre_act)
    active = pre_act * sigmoid_pre
    slopes = sigmoid_pre * (1.0 + pre_act * (1.0 - sigmoid_pre))
    curves = sigmoid_pre * (1.0 - sigmoid_pre) * (2.0 + pre_act * (1.0 - 2.0 * sigmoid_pre))
    return (active, slopes, curves)


def matmul(left, weight):
    return jnp.dot(left, weight, preferred_element_type=F32)


def matmul_trans(left, weight):
    return lax.dot_general(left, weight, (((1,), (1,)), ((), ())), preferred_element_type=F32)


def on_device(tokens, probe_words, token_ids, loss_weight, gate_weight, up_weight, down_weight):
    col, row = lax.axis_index("col"), lax.axis_index("row")
    core, hi, y = col % 2, (col // 2) % 2, col // 4
    lo, z = row % 2, row // 2
    width = gate_weight.shape[1]
    feats = tokens.shape[1]

    pair = jnp.stack([tokens, swap_lo(tokens)])
    pair = jnp.where(lo == 0, pair, pair[::-1])
    ring = gather_ring(pair, shift_z)
    ring = lax.dynamic_slice_in_dim(jnp.concatenate([ring, ring]), (4 - z) % 4, 4)
    words = probe_words.reshape(4, 2, 32, -1)

    def rows_for(k):
        tok = pick(ring, k, 1).reshape(128, feats)
        signs = unpack_signs(pick(words, k, 1).reshape(128, -1))
        return jnp.concatenate([tok, signs])

    theirs, mine = rows_for(1 - core), rows_for(core)

    def reduced_in(weight):
        arrived = swap_core(matmul(theirs, weight).astype(F16))
        both = (matmul(mine, weight) + arrived.astype(F32)).astype(F16)
        both = jnp.moveaxis(both.reshape(2, 4, 32, width), 1, 0)
        share = scatter_sum(both, shift_y, lambda d: (y + d) % 4, F16)
        share = share.reshape(2, 2, 16, width)
        other = swap_hi(pick(share, 1 - hi, 1).astype(F16))
        return pick(share, hi, 1) + other.astype(F32)

    gate_pre, gate_tan = reduced_in(gate_weight)
    up_pre, up_tan = reduced_in(up_weight)
    active, slopes, curves = silu_parts(gate_pre)
    hidden = (active * up_pre).astype(BF16)
    hidden_tan = (slopes * gate_tan * up_pre + active * up_tan).astype(BF16)

    def gathered_hidden(first, second):
        own = jnp.stack([first, second])
        own = jnp.stack([own, swap_hi(own)])
        own = gather_ring(own, shift_y)
        return jnp.stack([own, swap_core(own)], axis=1)

    def reduced_out(partial):
        share = scatter_sum(partial, shift_z, lambda d: (z + d - y) % 4, BF16)
        mine_at = (lo - core) % 2
        other = swap_lo(pick(share, 1 - mine_at).astype(BF16))
        total = pick(share, mine_at) + other.astype(F32)
        total = jnp.where(hi == 0, total, total[::-1])
        return jnp.moveaxis(total, 0, 1).reshape(-1, 32, feats)

    both = gathered_hidden(hidden, hidden_tan).reshape(512, width)
    output, out_tan = reduced_out(matmul(both, down_weight).reshape(4, 2, 2, 2, 16, feats))

    own_ids = lax.dynamic_slice_in_dim(token_ids, row * 32, 32)
    weight_tok = jnp.take(loss_weight, own_ids)[:, None]
    own_probe = unpack_signs(lax.dynamic_slice_in_dim(probe_words, row * 32, 32)).astype(F32)
    cotangent = (weight_tok * (tokens.astype(F32) + output)).astype(BF16)
    cot_tan = weight_tok * (own_probe + out_tan)

    own = jnp.stack([cotangent, cot_tan.astype(BF16)])
    own = jnp.stack([own, swap_lo(own)])
    cots = gather_ring(own, shift_z)
    theirs_at = (1 - core - lo) % 2
    cots_theirs = pick(cots, theirs_at, 1).reshape(256, feats)
    cots_mine = pick(cots, 1 - theirs_at, 1).reshape(256, feats)
    arrived = swap_core(matmul_trans(cots_theirs, down_weight).astype(BF16))
    back = matmul_trans(cots_mine, down_weight) + arrived.astype(F32)
    share = scatter_sum(back.reshape(4, 2, 32, width), shift_y, lambda d: (y + d - z) % 4, BF16)
    share = share.reshape(2, 2, 16, width)
    other = swap_hi(pick(share, 1 - hi, 1).astype(BF16))
    backward, back_tan = pick(share, hi, 1) + other.astype(F32)

    gate_back = (
        back_tan * up_pre * slopes
        + backward * up_tan * slopes
        + backward * up_pre * curves * gate_tan
    ).astype(BF16)
    up_back = (back_tan * active + backward * slopes * gate_tan).astype(BF16)
    both = gathered_hidden(gate_back, up_back)
    gates = both[:, :, :, 0].reshape(256, width)
    ups = both[:, :, :, 1].reshape(256, width)
    partial = matmul_trans(gates, gate_weight) + matmul_trans(ups, up_weight)
    summed = reduced_out(partial.reshape(4, 2, 2, 1, 16, feats))
    return cot_tan + summed[0]


def solution(mesh):
    return jax.shard_map(
        on_device,
        mesh=mesh,
        in_specs=(
            P("row", "col"),
            P(None, "col"),
            P(),
            P(),
            P("col", "row"),
            P("col", "row"),
            P("row", "col"),
        ),
        out_specs=P("row", "col"),
        check_vma=False,
    )
```

```python
import jax
import jax.numpy as jnp
from jax import lax
from jax.sharding import PartitionSpec as P


BF16 = jnp.bfloat16
F16 = jnp.float16
F32 = jnp.float32
STEPS = (1, 3, 2)
ROW_PEERS = [(1, 0), (3, 0), (2, 0), (0, 1), (1, 1), (3, 1), (2, 1)]


def shift_y(x, d):
    return lax.ppermute(x, "col", [(c, (c + 4 * d) % 16) for c in range(16)])


def shift_z(x, d):
    return lax.ppermute(x, "row", [(r, (r + 2 * d) % 8) for r in range(8)])


def send_row(x, step, flip):
    return lax.ppermute(x, "row", [(r, ((r + 2 * step) % 8) ^ flip) for r in range(8)])


def swap_core(x):
    return lax.ppermute(x, "col", [(c, c ^ 1) for c in range(16)])


def swap_hi(x):
    return lax.ppermute(x, "col", [(c, c ^ 2) for c in range(16)])


def swap_lo(x):
    return lax.ppermute(x, "row", [(r, r ^ 1) for r in range(8)])


def pick(x, i, axis=0):
    return lax.dynamic_index_in_dim(x, i, axis, keepdims=False)


def ring_sum(block, shift, narrow):
    arrived = [shift(block(d).astype(narrow), d) for d in STEPS]
    total = block(0).astype(F32)
    for a in arrived:
        total = total + a.astype(F32)
    return total


def pair_sum(own, sent, swap, narrow):
    return own.astype(F32) + swap(sent.astype(narrow)).astype(F32)


def from_ring(x, shift):
    got = {d: shift(x, d) for d in STEPS}
    return jnp.stack([x, got[3], got[2], got[1]])


def unpack_signs(packed):
    count = packed.shape[1]
    octets = [jnp.bitwise_and(jnp.right_shift(packed, 8 * b), 255) for b in range(4)]
    octets = jnp.concatenate(octets, axis=1).astype(BF16)
    source = lax.broadcasted_iota(jnp.int32, (4 * count, 32 * count), 0)
    feature = lax.broadcasted_iota(jnp.int32, (4 * count, 32 * count), 1)
    spread = (source == feature % 32 // 8 * count + feature // 32).astype(BF16)
    byte = jnp.dot(octets, spread, preferred_element_type=F32).astype(jnp.int32)
    place = lax.broadcasted_iota(jnp.int32, byte.shape, 1) % 8
    return (2 * jnp.bitwise_and(jnp.right_shift(byte, place), 1) - 1).astype(BF16)


def silu_parts(pre_act):
    sigmoid_pre = jax.nn.sigmoid(pre_act)
    active = pre_act * sigmoid_pre
    slopes = sigmoid_pre * (1.0 + pre_act * (1.0 - sigmoid_pre))
    curves = sigmoid_pre * (1.0 - sigmoid_pre) * (2.0 + pre_act * (1.0 - 2.0 * sigmoid_pre))
    return (active, slopes, curves)


def matmul(left, weight):
    return jnp.dot(left, weight, preferred_element_type=F32)


def matmul_trans(left, weight):
    return lax.dot_general(left, weight, (((1,), (1,)), ((), ())), preferred_element_type=F32)


def on_device(tokens, probe_words, token_ids, loss_weight, gate_weight, up_weight, down_weight):
    col, row = lax.axis_index("col"), lax.axis_index("row")
    core, hi, y = col % 2, (col // 2) % 2, col // 4
    lo, z = row % 2, row // 2
    width = gate_weight.shape[1]
    feats = tokens.shape[1]

    copies = jnp.broadcast_to(tokens, (8, *tokens.shape))
    every = lax.all_to_all(copies, "row", split_axis=0, concat_axis=0, tiled=True)
    every = every.reshape(4, 2, 2, 16, feats)
    probe = unpack_signs(probe_words)
    signs = probe.reshape(4, 2, 2, 16, feats)
    both = jnp.stack([every, signs], axis=3)
    rows = jnp.stack([pick(both, 1 - core, 1), pick(both, core, 1)])
    rows_hi = jnp.moveaxis(rows, 2, 1)

    def core_sums(rows, weight, product, narrow):
        theirs, mine = (r.reshape(256, feats) for r in (rows[0], rows[1]))
        arrived = swap_core(product(theirs, weight).astype(narrow))
        sums = product(mine, weight) + arrived.astype(F32)
        return sums.astype(narrow).reshape(*rows.shape[1:-1], width)

    def y_first(at, narrow):
        share = ring_sum(at, shift_y, narrow)
        return pair_sum(pick(share, hi), pick(share, 1 - hi), swap_hi, narrow)

    def hi_first(at, place, narrow):
        share = pair_sum(at(hi), at(1 - hi), swap_hi, narrow)
        return ring_sum(lambda d: pick(share, place(d)), shift_y, narrow)

    sums = core_sums(rows, gate_weight, matmul, F16)
    gate_pre, gate_tan = y_first(lambda d: pick(sums, (y + d) % 4), F16)
    sums_hi = core_sums(rows_hi, up_weight, matmul, F16)
    up_pre, up_tan = hi_first(lambda h: pick(sums_hi, h), lambda d: (y + d) % 4, F16)
    active, slopes, curves = silu_parts(gate_pre)
    hidden = (active * up_pre).astype(BF16)
    hidden_tan = (slopes * gate_tan * up_pre + active * up_tan).astype(BF16)

    def spread_hi_first(own):
        return from_ring(jnp.stack([own, swap_hi(own)]), shift_y)

    def spread_y_first(own):
        ring = from_ring(own, shift_y)
        return jnp.stack([ring, swap_hi(ring)], axis=1)

    def both_halves(half):
        half = half.reshape(128, width)
        return jnp.concatenate([half, swap_core(half)])

    shape = (2, 4, 2, 16, feats)
    parts = [
        matmul(both_halves(spread_hi_first(hidden)), down_weight).reshape(shape),
        matmul(both_halves(spread_y_first(hidden_tan)), down_weight).reshape(shape),
    ]

    def out_block(step, flip):
        half, at = ((lo ^ flip) != core).astype(jnp.int32), (z + step - y) % 4
        return jnp.stack([pick(pick(p, half), at) for p in parts])

    arrived = [send_row(out_block(*peer).astype(BF16), *peer) for peer in ROW_PEERS]
    total = out_block(0, 0)
    for a in arrived:
        total = total + a.astype(F32)
    output, out_tan = jnp.where(hi == 0, total, total[:, ::-1]).reshape(2, 32, feats)

    own_ids = lax.dynamic_slice_in_dim(token_ids, row * 32, 32)
    weight_tok = jnp.take(loss_weight, own_ids)[:, None]
    own_probe = lax.dynamic_slice_in_dim(probe, row * 32, 32).astype(F32)
    cotangent = (weight_tok * (tokens.astype(F32) + output)).astype(BF16)
    cot_tan = weight_tok * (own_probe + out_tan)

    cots = jnp.stack([cotangent, cot_tan.astype(BF16)])
    got = {(0, 0): cots}
    for step, flip in ROW_PEERS:
        got[((4 - step) % 4, flip)] = send_row(cots, step, flip)
    same = core == lo
    theirs = jnp.stack([jnp.where(same, got[d, 1], got[d, 0]) for d in range(4)], axis=1)
    mine = jnp.stack([jnp.where(same, got[d, 0], got[d, 1]) for d in range(4)], axis=1)
    arrived = swap_core(matmul_trans(theirs.reshape(256, feats), down_weight).astype(BF16))
    mine = matmul_trans(mine.reshape(256, feats), down_weight).reshape(2, 4, 2, 16, width)
    arrived = arrived.reshape(2, 4, 2, 16, width)

    def at_y(d):
        at = (y + d - z) % 4
        return pick(mine[0], at) + pick(arrived[0], at).astype(F32)

    def at_hi(h):
        return pick(mine[1], h, 1) + pick(arrived[1], h, 1).astype(F32)

    backward = y_first(at_y, BF16)
    back_tan = hi_first(at_hi, lambda d: (y + d - z) % 4, BF16)

    gate_back = (
        back_tan * up_pre * slopes
        + backward * up_tan * slopes
        + backward * up_pre * curves * gate_tan
    ).astype(BF16)
    up_back = (back_tan * active + backward * slopes * gate_tan).astype(BF16)
    gates = both_halves(spread_hi_first(gate_back))
    ups = both_halves(spread_y_first(up_back))
    partial = matmul_trans(gates, gate_weight) + matmul_trans(ups, up_weight)
    partial = partial.reshape(shape)
    share = ring_sum(lambda d: pick(partial, (z + d - y) % 4, 1), shift_z, BF16)
    at = (lo - core) % 2
    total = pair_sum(pick(share, at), pick(share, 1 - at), swap_lo, BF16)
    return cot_tan + jnp.where(hi == 0, total, total[::-1]).reshape(32, feats)


def solution(mesh):
    return jax.shard_map(
        on_device,
        mesh=mesh,
        in_specs=(
            P("row", "col"),
            P(None, "col"),
            P(),
            P(),
            P("col", "row"),
            P("col", "row"),
            P("row", "col"),
        ),
        out_specs=P("row", "col"),
        check_vma=False,
    )
```

```python
import jax
import jax.numpy as jnp
from jax import lax
from jax.sharding import PartitionSpec as P


BF16 = jnp.bfloat16
F16 = jnp.float16
F32 = jnp.float32
STEPS = (1, 3, 2)
ROW_PEERS = [(1, 0), (3, 0), (2, 0), (0, 1), (1, 1), (3, 1), (2, 1)]


def shift_y(x, d):
    return lax.ppermute(x, "col", [(c, (c + 4 * d) % 16) for c in range(16)])


def shift_z(x, d):
    return lax.ppermute(x, "row", [(r, (r + 2 * d) % 8) for r in range(8)])


def send_row(x, step, flip):
    return lax.ppermute(x, "row", [(r, ((r + 2 * step) % 8) ^ flip) for r in range(8)])


def from_row(x):
    copies = jnp.broadcast_to(x, (8, *x.shape))
    return lax.all_to_all(copies, "row", split_axis=0, concat_axis=0, tiled=True)


def swap_core(x):
    return lax.ppermute(x, "col", [(c, c ^ 1) for c in range(16)])


def swap_hi(x):
    return lax.ppermute(x, "col", [(c, c ^ 2) for c in range(16)])


def swap_lo(x):
    return lax.ppermute(x, "row", [(r, r ^ 1) for r in range(8)])


def pick(x, i, axis=0):
    return lax.dynamic_index_in_dim(x, i, axis, keepdims=False)


def ring_sum(block, shift, narrow):
    arrived = [shift(block(d).astype(narrow), d) for d in STEPS]
    total = block(0).astype(F32)
    for a in arrived:
        total = total + a.astype(F32)
    return total


def pair_sum(own, sent, swap, narrow):
    return own.astype(F32) + swap(sent.astype(narrow)).astype(F32)


def from_ring(x, shift):
    got = {d: shift(x, d) for d in STEPS}
    return jnp.stack([x, got[3], got[2], got[1]])


def unpack_signs(packed):
    count = packed.shape[1]
    octets = [jnp.bitwise_and(jnp.right_shift(packed, 8 * b), 255) for b in range(4)]
    octets = jnp.concatenate(octets, axis=1).astype(BF16)
    source = lax.broadcasted_iota(jnp.int32, (4 * count, 32 * count), 0)
    feature = lax.broadcasted_iota(jnp.int32, (4 * count, 32 * count), 1)
    spread = (source == feature % 32 // 8 * count + feature // 32).astype(BF16)
    byte = jnp.dot(octets, spread, preferred_element_type=F32).astype(jnp.int32)
    place = lax.broadcasted_iota(jnp.int32, byte.shape, 1) % 8
    return (2 * jnp.bitwise_and(jnp.right_shift(byte, place), 1) - 1).astype(BF16)


def silu_parts(pre_act):
    sigmoid_pre = jax.nn.sigmoid(pre_act)
    active = pre_act * sigmoid_pre
    slopes = sigmoid_pre * (1.0 + pre_act * (1.0 - sigmoid_pre))
    curves = sigmoid_pre * (1.0 - sigmoid_pre) * (2.0 + pre_act * (1.0 - 2.0 * sigmoid_pre))
    return (active, slopes, curves)


def matmul(left, weight):
    return jnp.dot(left, weight, preferred_element_type=F32)


def matmul_trans(left, weight):
    return lax.dot_general(left, weight, (((1,), (1,)), ((), ())), preferred_element_type=F32)


def on_device(tokens, probe_words, token_ids, loss_weight, gate_weight, up_weight, down_weight):
    col, row = lax.axis_index("col"), lax.axis_index("row")
    core, hi, y = col % 2, (col // 2) % 2, col // 4
    lo, z = row % 2, row // 2
    width = gate_weight.shape[1]
    feats = tokens.shape[1]

    every = from_row(tokens).reshape(4, 2, 2, 16, feats)
    probe = unpack_signs(probe_words)
    signs = probe.reshape(4, 2, 2, 16, feats)
    both = jnp.stack([every, signs], axis=3)
    rows = jnp.stack([pick(both, 1 - core, 1), pick(both, core, 1)])
    rows_hi = jnp.moveaxis(rows, 2, 1)

    def core_halves(rows, weight):
        halves = matmul(rows.reshape(512, feats), weight).astype(F16)
        halves = halves.reshape(*rows.shape[:-1], width)
        return halves[1], swap_core(halves[0])

    def both_at(halves, i):
        return pick(halves[0], i).astype(F32) + pick(halves[1], i).astype(F32)

    def y_first(at, narrow):
        share = ring_sum(at, shift_y, narrow)
        return pair_sum(pick(share, hi), pick(share, 1 - hi), swap_hi, narrow)

    def hi_first(at, narrow):
        share = pair_sum(at(hi), at(1 - hi), swap_hi, narrow)
        return ring_sum(lambda d: pick(share, (y + d) % 4), shift_y, narrow)

    gate_halves = core_halves(rows, gate_weight)
    gate_pre, gate_tan = y_first(lambda d: both_at(gate_halves, (y + d) % 4), F16)
    up_halves = core_halves(rows_hi, up_weight)
    up_pre, up_tan = hi_first(lambda h: both_at(up_halves, h), F16)
    active, slopes, curves = silu_parts(gate_pre)
    hidden = (active * up_pre).astype(BF16)
    hidden_tan = (slopes * gate_tan * up_pre + active * up_tan).astype(BF16)

    def spread_hi_first(own):
        return from_ring(jnp.stack([own, swap_hi(own)]), shift_y)

    def spread_y_first(own):
        ring = from_ring(own, shift_y)
        return jnp.stack([ring, swap_hi(ring)], axis=1)

    def both_halves(half):
        half = half.reshape(128, width)
        return jnp.concatenate([half, swap_core(half)])

    shape = (2, 4, 2, 16, feats)
    both = jnp.stack([both_halves(spread_hi_first(hidden)), both_halves(spread_y_first(hidden_tan))])
    parts = matmul(both.reshape(512, width), down_weight).reshape(2, *shape)

    def out_block(step, flip):
        half, at = ((lo ^ flip) != core).astype(jnp.int32), (z + step - y) % 4
        return pick(pick(parts, half, 1), at, 1)

    arrived = [send_row(out_block(*peer).astype(BF16), *peer) for peer in ROW_PEERS]
    total = out_block(0, 0)
    for a in arrived:
        total = total + a.astype(F32)
    output, out_tan = jnp.where(hi == 0, total, total[:, ::-1]).reshape(2, 32, feats)

    own_ids = lax.dynamic_slice_in_dim(token_ids, row * 32, 32)
    weight_tok = jnp.take(loss_weight, own_ids)[:, None]
    own_probe = lax.dynamic_slice_in_dim(probe, row * 32, 32).astype(F32)
    cotangent = (weight_tok * (tokens.astype(F32) + output)).astype(BF16)
    cot_tan = weight_tok * (own_probe + out_tan)

    cots = jnp.stack([cotangent, cot_tan.astype(BF16)])
    cots = from_row(cots).reshape(4, 2, 2, 32, feats)
    theirs, mine = (jnp.moveaxis(pick(cots, k, 1), 1, 0) for k in (1 - core, core))
    arrived = swap_core(matmul_trans(theirs.reshape(256, feats), down_weight).astype(BF16))
    mine = matmul_trans(mine.reshape(256, feats), down_weight).reshape(2, 4, 2, 16, width)
    arrived = arrived.reshape(2, 4, 2, 16, width)

    def at_y(d):
        at = (y + d) % 4
        return pick(mine[0], at) + pick(arrived[0], at).astype(F32)

    def at_hi(h):
        return pick(mine[1], h, 1) + pick(arrived[1], h, 1).astype(F32)

    backward = y_first(at_y, BF16)
    back_tan = hi_first(at_hi, BF16)

    gate_back = (
        back_tan * up_pre * slopes
        + backward * up_tan * slopes
        + backward * up_pre * curves * gate_tan
    ).astype(BF16)
    up_back = (back_tan * active + backward * slopes * gate_tan).astype(BF16)
    gates = both_halves(spread_hi_first(gate_back))
    ups = both_halves(spread_y_first(up_back))
    partial = matmul_trans(gates, gate_weight) + matmul_trans(ups, up_weight)
    partial = partial.reshape(shape)
    share = ring_sum(lambda d: pick(partial, (z + d - y) % 4, 1), shift_z, BF16)
    at = (lo - core) % 2
    total = pair_sum(pick(share, at), pick(share, 1 - at), swap_lo, BF16)
    return cot_tan + jnp.where(hi == 0, total, total[::-1]).reshape(32, feats)


def solution(mesh):
    return jax.shard_map(
        on_device,
        mesh=mesh,
        in_specs=(
            P("row", "col"),
            P(None, "col"),
            P(),
            P(),
            P("col", "row"),
            P("col", "row"),
            P("row", "col"),
        ),
        out_specs=P("row", "col"),
        check_vma=False,
    )
```
